8 devices in a mesh: dp: 2 (over y, z), tp: 4 (over x, core).
Axes of the slice: x: 2, y: 2, z: 1, core: 2. Of those that a mesh axis runs over, the one named last changes fastest.
Arguments:
- x: bfloat16 [2048, 4608], P(('dp', 'tp')), parts along dimension 0
- gain_a: bfloat16 [4608], replicated
- wq: bfloat16 [4608, 4096], P(None, 'tp')
- wk: bfloat16 [4608, 2048], P(None, 'tp')
- wv: bfloat16 [4608, 2048], P(None, 'tp')
- wo: bfloat16 [4096, 4608], P('tp')
- gain_m: bfloat16 [4608], replicated
- w_gate: bfloat16 [4608, 36864], P(None, 'tp')
- w_up: bfloat16 [4608, 36864], P(None, 'tp')
- w_down: bfloat16 [36864, 4608], P('tp')
Outputs:
- output: bfloat16 [2048, 4608], P(('dp', 'tp')), parts along dimension 0
There are 2 independent parts. The reference program is written for one: setup_inputs(seed, part) draws one part's arguments, and reference() takes and returns one part's arrays. A program takes and returns all parts, laid end to end along the dimension named above; an argument that names none is the same for every part.
All inputs are finite; a program needn't handle non-finite values.
Results may differ from the reference program's by a relative error of at most 0.017.
Values are sent between devices in bfloat16 or wider.
A program may use at most 2 GiB of HBM per device.

```python
import jax
import jax.numpy as jnp
from jax import lax

ROWS = 1024
D = 4608
HEADS = 32
KV_HEADS = 16
HEAD = 128
FF = 36864
THETA = 10000


def setup_inputs(seed: int = 0, part: int = 0) -> dict:
    kx, kn, kq, kk, kv, ko, km, kg, ku, kd = jax.random.split(jax.random.key(seed), 10)

    def weights(key, rows, columns):
        return jax.random.normal(key, (rows, columns), jnp.float32) * rows**-0.5

    drawn = {
        "x": jax.random.normal(jax.random.fold_in(kx, part), (ROWS, D), jnp.float32),
        "gain_a": 1 + 0.1 * jax.random.normal(kn, (D,), jnp.float32),
        "wq": 2 * weights(kq, D, HEADS * HEAD),
        "wk": 2 * weights(kk, D, KV_HEADS * HEAD),
        "wv": 4 * weights(kv, D, KV_HEADS * HEAD),
        "wo": weights(ko, HEADS * HEAD, D),
        "gain_m": 1 + 0.1 * jax.random.normal(km, (D,), jnp.float32),
        "w_gate": weights(kg, D, FF),
        "w_up": weights(ku, D, FF),
        "w_down": 2 * weights(kd, FF, D),
    }
    return {k: v.astype(jnp.bfloat16) for k, v in drawn.items()}


def normed(x, gain):
    wide = x.astype(jnp.float32)
    scale = lax.rsqrt(jnp.mean(wide * wide, -1, keepdims=True) + 1e-6)
    return (wide * scale * gain.astype(jnp.float32)).astype(jnp.bfloat16)


def turned(t, place, theta):
    half = t.shape[-1] // 2
    angle = place.astype(jnp.float32)[:, None] * theta ** (-jnp.arange(half, dtype=jnp.float32) / half)
    cos, sin = jnp.cos(angle)[:, None], jnp.sin(angle)[:, None]
    a, b = t[..., :half].astype(jnp.float32), t[..., half:].astype(jnp.float32)
    return jnp.concatenate([a * cos - b * sin, b * cos + a * sin], -1).astype(jnp.bfloat16)


def matmul(a, w):
    return jnp.dot(a, w, preferred_element_type=jnp.float32).astype(jnp.bfloat16)


def einsum(form, a, b):
    return jnp.einsum(form, a.astype(jnp.float32), b.astype(jnp.float32))


def attention(q, k, v):
    scores = einsum("tgsd,ugd->gstu", q, k) * q.shape[-1] ** -0.5
    token = jnp.arange(q.shape[0])
    scores = jnp.where(token[:, None] >= token, scores, -jnp.inf)
    weights = jax.nn.softmax(scores, -1).astype(jnp.bfloat16)
    return einsum("gstu,ugd->tgsd", weights, v).astype(jnp.bfloat16)


def reference(x, gain_a, wq, wk, wv, wo, gain_m, w_gate, w_up, w_down):
    a, place = normed(x, gain_a), jnp.arange(ROWS)
    q = turned(matmul(a, wq).reshape(ROWS, HEADS, HEAD), place, THETA).reshape(ROWS, KV_HEADS, -1, HEAD)
    k = turned(matmul(a, wk).reshape(ROWS, KV_HEADS, HEAD), place, THETA)
    v = matmul(a, wv).reshape(ROWS, KV_HEADS, HEAD)
    seen = attention(q, k, v).reshape(ROWS, HEADS * HEAD)
    h = (x.astype(jnp.float32) + jnp.dot(seen, wo, preferred_element_type=jnp.float32)).astype(jnp.bfloat16)
    b = normed(h, gain_m)
    gate = jnp.dot(b, w_gate, preferred_element_type=jnp.float32)
    up = jnp.dot(b, w_up, preferred_element_type=jnp.float32)
    hidden = (jax.nn.silu(gate) * up).astype(jnp.bfloat16)
    return (h.astype(jnp.float32) + jnp.dot(hidden, w_down, preferred_element_type=jnp.float32)).astype(jnp.bfloat16)
```

```python
import functools

import jax
import jax.numpy as jnp
from jax import lax
from jax.experimental import pallas as pl
from jax.experimental.pallas import tpu as pltpu
from jax.sharding import PartitionSpec as P

HEAD = 128
THETA = 10000
BLOCK = 256
NEG = -1e30
LOG2E = 1.4426950408889634
VMEM = 60 * 2**20
BF, F32 = jnp.bfloat16, jnp.float32


def _params(*semantics):
    return pltpu.CompilerParams(dimension_semantics=semantics, vmem_limit_bytes=VMEM)


def _dot(a, b, ca=1, cb=0):
    return lax.dot_general(a, b, (((ca,), (cb,)), ((), ())), preferred_element_type=F32)


def _whole(shape):
    return pl.BlockSpec(shape, lambda *_: (0,) * len(shape))


def _norm_kernel(x_ref, g_ref, o_ref):
    wide = x_ref[...].astype(F32)
    scale = lax.rsqrt(jnp.mean(wide * wide, -1, keepdims=True) + 1e-6)
    o_ref[...] = (wide * scale * g_ref[...].astype(F32)).astype(BF)


def norm(x, gain):
    rows, d = x.shape
    return pl.pallas_call(
        _norm_kernel, grid=(rows // 64,), name="norm",
        in_specs=[pl.BlockSpec((64, d), lambda i: (i, 0)), _whole((1, d))],
        out_specs=pl.BlockSpec((64, d), lambda i: (i, 0)),
        out_shape=jax.ShapeDtypeStruct((rows, d), BF),
        compiler_params=_params("arbitrary"),
        cost_estimate=pl.CostEstimate(flops=rows * d * 8, bytes_accessed=rows * d * 4, transcendentals=rows),
    )(x, gain[None])


def _turn(t, cos, sin):
    heads = []
    for i in range(t.shape[1] // HEAD):
        u = t[:, i * HEAD : (i + 1) * HEAD]
        heads.append(u * cos + pltpu.roll(u, HEAD // 2, 1) * sin)
    return jnp.concatenate(heads, 1)


def _qkv_kernel(a_ref, b_ref, cos_ref, sin_ref, wq_ref, wk_ref, wv_ref, q_ref, k_ref, v_ref, some):
    j = pl.program_id(0)

    @pl.when(j == 0)
    def _():
        some[:BLOCK] = a_ref[...]
        some[BLOCK:] = b_ref[...]

    @pl.when(j < 4)
    def _():
        t = _dot(some[...], wq_ref[...]).astype(BF).astype(F32)
        q_ref[...] = _turn(t, cos_ref[...], sin_ref[...]).astype(BF)

    @pl.when((j >= 4) & (j < 6))
    def _():
        t = _dot(some[...], wk_ref[...]).astype(BF).astype(F32)
        k_ref[...] = _turn(t, cos_ref[...], sin_ref[...]).astype(BF)

    @pl.when(j >= 6)
    def _():
        v_ref[...] = _dot(some[...], wv_ref[...]).astype(BF)


def qkv(a, b, cos, sin, wq, wk, wv):
    d = a.shape[1]
    rows, w = 2 * BLOCK, 256
    q_at = lambda j: (0, jnp.minimum(j, 3))
    k_at = lambda j: (0, jnp.clip(j - 4, 0, 1))
    v_at = lambda j: (0, jnp.clip(j - 6, 0, 1))
    return pl.pallas_call(
        _qkv_kernel, grid=(8,), name="qkv",
        in_specs=[_whole((BLOCK, d)), _whole((BLOCK, d)), _whole((rows, HEAD)), _whole((rows, HEAD)),
                  pl.BlockSpec((d, w), q_at), pl.BlockSpec((d, w), k_at), pl.BlockSpec((d, w), v_at)],
        out_specs=[pl.BlockSpec((rows, w), q_at), pl.BlockSpec((rows, w), k_at), pl.BlockSpec((rows, w), v_at)],
        out_shape=[jax.ShapeDtypeStruct((rows, n), BF) for n in (wq.shape[1], wk.shape[1], wv.shape[1])],
        scratch_shapes=[pltpu.VMEM((rows, d), BF)],
        compiler_params=_params("arbitrary"),
        cost_estimate=pl.CostEstimate(flops=2 * rows * d * 2048, bytes_accessed=(rows * d + d * 2048) * 2, transcendentals=0),
    )(a, b, cos, sin, wq, wk, wv)


def _attend_kernel(t_ref, q_ref, ka_ref, kb_ref, va_ref, vb_ref, o_ref, k_s, v_s, top_s, mix_s):
    r, t = pl.program_id(0), t_ref[0]
    groups, g = k_s.shape[1] // HEAD, q_ref.shape[1] // k_s.shape[1]
    cols = g * BLOCK
    e = HEAD**-0.5 * LOG2E

    @pl.when(r == 0)
    def _():
        k_s[: 2 * BLOCK], k_s[2 * BLOCK :] = ka_ref[...], kb_ref[...]
        v_s[: 2 * BLOCK], v_s[2 * BLOCK :] = va_ref[...], vb_ref[...]

    top_s[...] = jnp.full(top_s.shape, NEG, F32)
    mix_s[...] = jnp.zeros(mix_s.shape, F32)
    q = [jnp.concatenate([q_ref[:, (g * i + n) * HEAD : (g * i + n + 1) * HEAD] for n in range(g)], 0) for i in range(groups)]
    ones = jnp.ones((8, BLOCK), BF)

    def block(at, masked):
        here = pl.ds(pl.multiple_of(at * BLOCK, BLOCK), BLOCK)
        scores = [_dot(k_s[here, i * HEAD : (i + 1) * HEAD], q[i], 1, 1) for i in range(groups)]
        if masked:
            gap = lax.broadcasted_iota(jnp.int32, (BLOCK, cols), 1) % BLOCK - lax.broadcasted_iota(jnp.int32, (BLOCK, cols), 0)
        weights, keeps = [], []
        for i, s in enumerate(scores):
            if masked:
                s = jnp.where(gap >= 0, s, 2 * NEG)
            old = top_s[i : i + 1, :]
            top = jnp.maximum(old, s.max(axis=0, keepdims=True))
            top_s[i : i + 1, :] = top
            weights.append(jnp.exp2((s - top) * e).astype(BF))
            keeps.append(jnp.exp2((old - top) * e))
        for i, (p, keep) in enumerate(zip(weights, keeps)):
            values = jnp.concatenate([v_s[here, i * HEAD : (i + 1) * HEAD].T, ones], axis=0)
            mix_s[i] = mix_s[i] * keep + _dot(values, p)

    lax.fori_loop(0, r ^ t, lambda b, _: block(b ^ t, False), None)
    block(r, True)
    for i in range(groups):
        out = (mix_s[i, :HEAD, :] * (1 / mix_s[i, HEAD : HEAD + 1, :])).T.astype(BF)
        for n in range(g):
            o_ref[:, (g * i + n) * HEAD : (g * i + n + 1) * HEAD] = out[n * BLOCK : (n + 1) * BLOCK]


def attend(t, q, ka, kb, va, vb):
    rows, wide = q.shape
    kw = ka.shape[1]
    g = wide // kw
    return pl.pallas_call(
        _attend_kernel, name="attend",
        grid_spec=pltpu.PrefetchScalarGridSpec(
            num_scalar_prefetch=1, grid=(rows // BLOCK,),
            in_specs=[pl.BlockSpec((BLOCK, wide), lambda r, _: (r, 0))] + [_whole((2 * BLOCK, kw))] * 4,
            out_specs=pl.BlockSpec((BLOCK, wide), lambda r, _: (r, 0)),
            scratch_shapes=[pltpu.VMEM((4 * BLOCK, kw), BF), pltpu.VMEM((4 * BLOCK, kw), BF), pltpu.VMEM((kw // HEAD, g * BLOCK), F32),
                            pltpu.VMEM((kw // HEAD, HEAD + 8, g * BLOCK), F32)],
        ),
        out_shape=jax.ShapeDtypeStruct((rows, wide), BF),
        compiler_params=_params("arbitrary"),
        cost_estimate=pl.CostEstimate(flops=4 * rows * rows * wide, bytes_accessed=rows * wide * 6, transcendentals=rows * rows * 8),
    )(t, q, ka, kb, va, vb)


def _mm2_kernel(x_ref, w_ref, keep_ref, give_ref):
    y = _dot(x_ref[...], w_ref[...]).astype(BF)
    keep_ref[...] = y[:BLOCK]
    give_ref[...] = y[BLOCK:]


def mm2(x, w, part, first, count, width, name):
    k = x.shape[1]
    out = jax.ShapeDtypeStruct((BLOCK, count * width), BF)
    return pl.pallas_call(
        _mm2_kernel, grid=(count,), name=name,
        in_specs=[pl.BlockSpec((2 * BLOCK, k), lambda j: (part, 0)), pl.BlockSpec((k, width), lambda j: (0, first + j))],
        out_specs=[pl.BlockSpec((BLOCK, width), lambda j: (0, j))] * 2,
        out_shape=[out, out],
        compiler_params=_params("arbitrary"),
        cost_estimate=pl.CostEstimate(flops=4 * BLOCK * k * count * width, bytes_accessed=(2 * BLOCK * k + k * count * width) * 2, transcendentals=0),
    )(x, w)


WIDE = 512


def _neighbours():
    t = lax.axis_index("tp")
    sib = t + 1 - 2 * (t % 2)
    far = (t + 2) % 4
    return sib, far


def _mlp_kernel(h_ref, gain_ref, wg_ref, wu_ref, wd_ref, o_ref, some, hidden, w, recv, got, sums, give, keep, h_s, out_s,
                h_sem, w_sem, o_sem, gat_send, gat_recv, give_send, recv_sem, sum_send, got_sem):
    d = h_s.shape[1]
    ups, downs = wg_ref.shape[1] // WIDE, d // WIDE
    sib, far = _neighbours()

    def remote(src, dst, send, receive, to):
        return pltpu.make_async_remote_copy(src_ref=src, dst_ref=dst, send_sem=send, recv_sem=receive, device_id={"tp": to},
                                            device_id_type=pl.DeviceIdType.MESH)

    def tiles_up(s, p):
        at = pl.ds(pl.multiple_of((s % ups) * WIDE, WIDE), WIDE)
        return (pltpu.make_async_copy(wg_ref.at[:, at], w.at[2 * p], w_sem.at[2 * p]),
                pltpu.make_async_copy(wu_ref.at[:, at], w.at[2 * p + 1], w_sem.at[2 * p + 1]))

    def tiles_down(s, p):
        at = pl.ds(pl.multiple_of((s % downs) * WIDE, WIDE), WIDE)
        return (pltpu.make_async_copy(wd_ref.at[pl.ds(0, d), at], w.at[2 * p], w_sem.at[2 * p]),
                pltpu.make_async_copy(wd_ref.at[pl.ds(d, d), at], w.at[2 * p + 1], w_sem.at[2 * p + 1]))

    load = pltpu.make_async_copy(h_ref, h_s, h_sem)
    load.start()
    for copy in tiles_up(0, 0):
        copy.start()
    barrier = pltpu.get_barrier_semaphore()
    for to in (sib, far):
        pl.semaphore_signal(barrier, inc=1, device_id={"tp": to}, device_id_type=pl.DeviceIdType.MESH)
    load.wait()
    gain = gain_ref[...].astype(F32)

    def norm_rows(i, _):
        at = pl.ds(pl.multiple_of(i * 32, 32), 32)
        wide = h_s[at].astype(F32)
        scale = lax.rsqrt(jnp.mean(wide * wide, -1, keepdims=True) + 1e-6)
        some[at] = (wide * scale * gain).astype(BF)

    lax.fori_loop(0, BLOCK // 32, norm_rows, None)
    pl.semaphore_wait(barrier, 2)
    block = lambda i: some.at[pl.ds(i * BLOCK, BLOCK)]
    to_sib = remote(block(0), block(1), gat_send.at[0], gat_recv.at[0], sib)
    to_far = remote(block(0), block(2), gat_send.at[1], gat_recv.at[1], far)
    on = remote(block(2), block(3), gat_send.at[2], gat_recv.at[2], sib)
    to_sib.start()
    to_far.start()
    to_sib.wait_recv()

    def up_step(s, _):
        p = s % 2
        for copy in tiles_up(s, p):
            copy.wait()

        @pl.when(s + 1 < 2 * ups)
        def _():
            for copy in tiles_up(s + 1, 1 - p):
                copy.start()

        @pl.when(s + 1 == 2 * ups)
        def _():
            for copy in tiles_down(0, 1 - p):
                copy.start()

        @pl.when(s == ups - 4)
        def _():
            to_far.wait_recv()
            on.start()

        @pl.when(s == ups)
        def _():
            on.wait_recv()

        rows = pl.ds(pl.multiple_of((s // ups) * (2 * BLOCK), 2 * BLOCK), 2 * BLOCK)
        x = some[rows]
        gate, up = _dot(x, w[2 * p]), _dot(x, w[2 * p + 1])
        hidden[rows, pl.ds(pl.multiple_of((s % ups) * WIDE, WIDE), WIDE)] = (jax.nn.silu(gate) * up).astype(BF)

    lax.fori_loop(0, 2 * ups, up_step, None)

    def give_copy(s):
        return remote(give.at[s % 2], recv.at[s], give_send.at[s % 2], recv_sem.at[s], sib)

    def sum_copy(n):
        return remote(sums.at[n % 3], got.at[n], sum_send.at[n % 3], got_sem.at[n], far)

    def out_copy(n):
        at = pl.ds(pl.multiple_of(n * WIDE, WIDE), WIDE)
        return pltpu.make_async_copy(out_s.at[n % 2], o_ref.at[:, at], o_sem.at[n % 2])

    def finish(s):
        give_copy(s).wait_recv()

        @pl.when(s < downs)
        def _():
            @pl.when(s >= 3)
            def _():
                sum_copy(s - 3).wait_send()

            sums[s % 3] = (keep[s % 2] + recv[s].astype(F32)).astype(BF)
            sum_copy(s).start()

        @pl.when(s >= downs)
        def _():
            n = s - downs

            @pl.when(n >= 2)
            def _():
                out_copy(n - 2).wait()

            sum_copy(n).wait_recv()
            at = pl.ds(pl.multiple_of(n * WIDE, WIDE), WIDE)
            out_s[n % 2] = (h_s[:, at].astype(F32) + keep[s % 2] + recv[s].astype(F32) + got[n].astype(F32)).astype(BF)
            out_copy(n).start()

    def down_step(s, _):
        p = s % 2
        for copy in tiles_down(s, p):
            copy.wait()

        @pl.when(s + 1 < 2 * downs)
        def _():
            for copy in tiles_down(s + 1, 1 - p):
                copy.start()

        @pl.when(s >= 1)
        def _():
            finish(s - 1)

        @pl.when(s >= 2)
        def _():
            give_copy(s - 2).wait_send()

        rows = pl.ds(pl.multiple_of((1 - s // downs) * (2 * BLOCK), 2 * BLOCK), 2 * BLOCK)
        y = _dot(hidden[rows, :d], w[2 * p]) + _dot(hidden[rows, d:], w[2 * p + 1])
        give[s % 2] = y[BLOCK:].astype(BF)
        keep[s % 2] = y[:BLOCK]
        give_copy(s).start()

    lax.fori_loop(0, 2 * downs, down_step, None)
    finish(2 * downs - 1)
    for n in range(downs - 2, downs):
        out_copy(n).wait()
    for s in range(2 * downs - 2, 2 * downs):
        give_copy(s).wait_send()
    for n in range(downs - 3, downs):
        sum_copy(n).wait_send()
    for copy in (to_sib, to_far, on):
        copy.wait_send()


def mlp(h, gain, wg, wu, wd):
    d, n = wg.shape
    downs = d // WIDE
    dma = pltpu.SemaphoreType.DMA
    any_ = pl.BlockSpec(memory_space=pl.ANY)
    return pl.pallas_call(
        _mlp_kernel, name="mlp",
        in_specs=[any_, pl.BlockSpec(memory_space=pltpu.VMEM), any_, any_, any_],
        out_specs=any_,
        out_shape=jax.ShapeDtypeStruct((BLOCK, d), BF),
        scratch_shapes=[
            pltpu.VMEM((4 * BLOCK, d), BF), pltpu.VMEM((4 * BLOCK, n), BF), pltpu.VMEM((4, d, WIDE), BF),
            pltpu.VMEM((2 * downs, BLOCK, WIDE), BF), pltpu.VMEM((downs, BLOCK, WIDE), BF), pltpu.VMEM((3, BLOCK, WIDE), BF),
            pltpu.VMEM((2, BLOCK, WIDE), BF), pltpu.VMEM((2, BLOCK, WIDE), F32), pltpu.VMEM((BLOCK, d), BF), pltpu.VMEM((2, BLOCK, WIDE), BF),
            dma(()), dma((4,)), dma((2,)), dma((3,)), dma((3,)), dma((2,)), dma((2 * downs,)), dma((3,)), dma((downs,)),
        ],
        compiler_params=pltpu.CompilerParams(collective_id=1, has_side_effects=True, vmem_limit_bytes=63 * 2**20),
        cost_estimate=pl.CostEstimate(flops=24 * BLOCK * d * n, bytes_accessed=12 * d * n, transcendentals=4 * BLOCK * n),
    )(h, gain[None], wg, wu, wd)


S_PAIRS = [(0, 1), (1, 0), (2, 3), (3, 2)]
X_PAIRS = [(0, 2), (2, 0), (1, 3), (3, 1)]


def solution(mesh):
    def S(t):
        return lax.ppermute(t, "tp", S_PAIRS)

    def X(t):
        return lax.ppermute(t, "tp", X_PAIRS)

    def after(t, *done):
        return lax.optimization_barrier((t, *done))[0]

    def add(a, b):
        return (a.astype(F32) + b.astype(F32)).astype(BF)

    def step(x, gain_a, wq, wk, wv, wo, gain_m, w_gate, w_up, w_down):
        t = lax.axis_index("tp")
        half = HEAD // 2
        place = (jnp.bitwise_xor(jnp.arange(4), t)[:, None] * BLOCK + jnp.arange(BLOCK)).reshape(-1)
        angle = place.astype(F32)[:, None] * THETA ** (-jnp.arange(half, dtype=F32) / half)
        cos, sin = jnp.cos(angle), jnp.sin(angle)
        cos, sin = jnp.concatenate([cos, cos], 1), jnp.concatenate([-sin, sin], 1)
        two = 2 * BLOCK

        a = norm(x, gain_a)
        ax, as_ = X(a), S(a)
        q0, k0, v0 = qkv(a, as_, cos[:two], sin[:two], wq, wk, wv)
        ax = after(ax, q0)
        axs = S(ax)
        q1, k1, v1 = qkv(ax, axs, cos[two:], sin[two:], wq, wk, wv)
        seen = attend(t.reshape(1), jnp.concatenate([q0, q1]), k0, k1, v0, v1)
        keep, give = mm2(seen, wo, 1, 0, 9, 512, "wo_far")
        got = X(add(keep, S(give)))
        keep, give = mm2(seen, wo, 0, 0, 9, 512, "wo_near")
        h = (x.astype(F32) + keep.astype(F32) + S(give).astype(F32) + got.astype(F32)).astype(BF)

        return mlp(h, gain_m, w_gate, w_up, w_down)

    tokens, columns, rows_of = P(("dp", "tp"), None), P(None, "tp"), P("tp", None)
    return jax.shard_map(
        step,
        mesh=mesh,
        in_specs=(tokens, P(None), columns, columns, columns, rows_of, P(None), columns, columns, rows_of),
        out_specs=tokens,
        check_vma=False,
    )
```

```python
import jax
import jax.numpy as jnp
import numpy as np
from jax import lax
from jax.experimental import pallas as pl
from jax.experimental.pallas import tpu as pltpu
from jax.sharding import PartitionSpec as P

HEAD = 128
THETA = 10000
BLOCK = 256
HALF = 128
WIDE = 512
NEG = -1e30
LOG2E = 1.4426950408889634
BF, F32 = jnp.bfloat16, jnp.float32


SWAP, A_OVER, A_ON, FAR_GIVE, SUM, NEAR_GIVE, B_SIB, B_OVER, B_ON, H_SWAP, DOWN_GIVE, DOWN_SUM = 0, 3, 5, 7, 9, 15, 17, 19, 21, 23, 24, 42
COPIES = 51


def _dot(a, b, ca=1, cb=0):
    return lax.dot_general(a, b, (((ca,), (cb,)), ((), ())), preferred_element_type=F32)


def _ds(at, size, unit=None):
    return pl.ds(at if isinstance(at, int) else pl.multiple_of(at, unit or size), size)


def _kernel(x_ref, ga_ref, tab_ref, wq_ref, wk_ref, wv_ref, wo_ref, gm_ref, wg_ref, wu_ref, wd_ref, o_ref,
            some, hidden, w, recv, got, keep, x_s, tab_s, top_s, total_s, x_sem, w_sem, wo_sem, tab_sem, o_sem, send_sem, recv_sem):
    d = some.shape[1]
    ups, downs = wg_ref.shape[1] // WIDE, d // WIDE
    QC, KC, VC, SC, TC = d, d + 1024, d + 1536, d + 2048, d + 3072
    t = lax.axis_index("tp")
    c, chip = t % 2, t // 2
    sib, far = t + 1 - 2 * c, (t + 2) % 4

    def row(side, b, half=0):
        return side * 2 * BLOCK + ((b + c) % 2) * BLOCK + half * HALF

    def sib_row(side, b, half=0):
        return side * 2 * BLOCK + ((b + 1 + c) % 2) * BLOCK + half * HALF

    def remote(i, src, dst, to):
        return pltpu.make_async_remote_copy(src_ref=src, dst_ref=dst, send_sem=send_sem.at[i], recv_sem=recv_sem.at[i], device_id={"tp": to},
                                            device_id_type=pl.DeviceIdType.MESH)

    def rows(ref, at, size=HALF):
        return ref.at[_ds(at, size, HALF)]

    load = pltpu.make_async_copy(x_ref, x_s.at[pl.ds(0, BLOCK)], x_sem)
    load.start()
    in_weights = [pltpu.make_async_copy(src, w.at[i], w_sem.at[i]) for i, src in
                  enumerate((wq_ref.at[:, pl.ds(0, WIDE)], wq_ref.at[:, pl.ds(WIDE, WIDE)], wk_ref, wv_ref))]
    for copy in in_weights:
        copy.start()
    wo_copy = pltpu.make_async_copy(wo_ref, hidden.at[:, pl.ds(0, d)], wo_sem)
    wo_copy.start()
    barrier = pltpu.get_barrier_semaphore()
    for to in (sib, far):
        pl.semaphore_signal(barrier, inc=1, device_id={"tp": to}, device_id_type=pl.DeviceIdType.MESH)
    load.wait()

    def norm_rows(gain_ref, src, dst):
        gain = gain_ref[...].astype(F32)[None]

        def go(i, _):
            wide = x_s[_ds(src + i * 32, 32)].astype(F32)
            scale = lax.rsqrt(jnp.mean(wide * wide, -1, keepdims=True) + 1e-6)
            some[_ds(dst + i * 32, 32)] = (wide * scale * gain).astype(BF)

        lax.fori_loop(0, HALF // 32, go, None)

    other, mine = (1 - c) * HALF, c * HALF
    swap = [remote(SWAP, rows(some, other), rows(some, BLOCK + other), sib),
            remote(SWAP + 1, rows(some, mine), rows(some, BLOCK + mine), sib),
            remote(SWAP + 2, rows(x_s, other), rows(x_s, BLOCK), sib)]

    def a_over(b):
        return remote(A_OVER + b, rows(some, row(0, b, c)), rows(some, row(1, b, c)), far)

    def a_on(b):
        return remote(A_ON + b, rows(some, row(1, b, c)), rows(some, sib_row(1, b, c)), sib)

    norm_rows(ga_ref, other, other)
    pl.semaphore_wait(barrier, 2)
    swap[0].start()
    norm_rows(ga_ref, mine, mine)

    @pl.when(c == 0)
    def _():
        a_over(0).start()

    swap[1].start()
    swap[2].start()
    swap[0].wait_recv()

    @pl.when(c == 1)
    def _():
        a_over(0).start()

    a_over(1).start()

    def table_copy(i):
        place = ((chip + i // 2) % 2) * 2 + i % 2
        return pltpu.make_async_copy(tab_ref.at[_ds(place * BLOCK, BLOCK)], tab_s, tab_sem)

    def qkv(side, b):
        at = _ds(row(side, b), BLOCK)
        table_copy(side * 2 + b).wait()
        table = tab_s[...]
        turned = pltpu.roll(table, HEAD // 2, 1)
        first = lax.broadcasted_iota(jnp.int32, table.shape, 1) < HEAD // 2
        cos, sin = jnp.where(first, table, turned), jnp.where(first, -turned, table)
        for i, to in enumerate((QC, QC + WIDE, KC, VC)):
            y = _dot(some[at], w[i]).astype(BF)
            if i < 3:
                heads = []
                for n in range(WIDE // HEAD):
                    u = y[:, n * HEAD : (n + 1) * HEAD].astype(F32)
                    heads.append((u * cos + pltpu.roll(u, HEAD // 2, 1) * sin).astype(BF))
                y = jnp.concatenate(heads, 1)
            hidden[at, to : to + WIDE] = y

        @pl.when(side * 2 + b < 3)
        def _():
            table_copy(side * 2 + b + 1).start()

    groups, g = WIDE // HEAD, 2
    cols = g * BLOCK
    e = HEAD**-0.5 * LOG2E
    ones = jnp.ones((8, BLOCK), BF)

    def attend(side, b, kept, given):
        at = _ds(row(side, b), BLOCK)
        top_s[...] = jnp.full(top_s.shape, NEG, F32)
        total_s[...] = jnp.zeros(total_s.shape, F32)
        keep[...] = jnp.zeros(keep.shape, F32)

        def block(key_row, masked):
            here = _ds(key_row, BLOCK)
            weights, shrinks = [], []
            for i in range(groups):
                q = jnp.concatenate([hidden[at, QC + (g * i + n) * HEAD : QC + (g * i + n + 1) * HEAD] for n in range(g)], 0)
                s = _dot(hidden[here, KC + i * HEAD : KC + (i + 1) * HEAD], q, 1, 1)
                if masked:
                    gap = lax.broadcasted_iota(jnp.int32, s.shape, 1) % BLOCK - lax.broadcasted_iota(jnp.int32, s.shape, 0)
                    s = jnp.where(gap >= 0, s, 2 * NEG)
                old = top_s[i : i + 1, :]
                top = jnp.maximum(old, s.max(axis=0, keepdims=True))
                top_s[i : i + 1, :] = top
                weights.append(jnp.exp2((s - top) * e).astype(BF))
                shrinks.append(jnp.exp2((old - top) * e))
            for i, (p, shrink) in enumerate(zip(weights, shrinks)):
                values = jnp.concatenate([hidden[here, VC + i * HEAD : VC + (i + 1) * HEAD].T, ones], axis=0)
                more = _dot(values, p)
                to = slice((i % 2) * HEAD, (i % 2 + 1) * HEAD)
                keep[i // 2, to] = keep[i // 2, to] * shrink + more[:HEAD]
                total_s[i] = total_s[i] * shrink + more[HEAD:]

        before = 2 * (1 - chip) if side else 2 * chip

        def whole(j, _):
            there = (before // 2) * (1 - j // 2)
            block(there * ((1 - side) * 2 * BLOCK + j * BLOCK) + (1 - there) * row(side, 0), False)

        lax.fori_loop(0, before + b, whole, None)
        block(row(side, b), True)
        for i in range(groups):
            out = (keep[i // 2, (i % 2) * HEAD : (i % 2 + 1) * HEAD] * (1 / total_s[i, :1])).T.astype(BF)
            for n in range(g):
                to = slice(SC + (g * i + n) * HEAD, SC + (g * i + n + 1) * HEAD)
                for half in range(2):
                    piece = out[n * BLOCK + half * HALF : n * BLOCK + (half + 1) * HALF]
                    hidden[_ds(kept + ((half + c) % 2) * (given - kept), HALF), to] = piece

    def out_dot(at, size, n):
        return _dot(hidden[at : at + size, SC : SC + 1024], hidden[:, _ds(n * WIDE, WIDE)])

    table_copy(0).start()
    for copy in in_weights:
        copy.wait()
    swap[1].wait_recv()
    lax.fori_loop(0, 2, lambda b, _: qkv(0, b), None)
    for copy in swap:
        copy.wait_send()

    def far_give(b):
        return remote(FAR_GIVE + b, rows(some, row(1, b, 1 - c)), rows(recv.at[0], b * HALF), sib)

    near_give = [remote(NEAR_GIVE + b, rows(some, row(0, b, c)), rows(recv.at[1], b * HALF), sib) for b in range(2)]
    third = downs // 3

    def sum_over(b, i):
        part = pl.ds(i * third * WIDE, third * WIDE)
        return remote(SUM + 3 * b + i, hidden.at[_ds((3 * b + i) * HALF, HALF), pl.ds(TC, third * WIDE)], got.at[_ds(b * HALF, HALF), part], far)

    def far_block(b, _):
        a_over(b).wait_recv()
        a_on(b).start()
        a_on(b).wait_recv()
        qkv(1, b)
        a_on(b).wait_send()

        @pl.when(b == 1)
        def _():
            for copy in tiles_up(wg_ref, wu_ref, w, w_sem, ups, 0, 0):
                copy.start()

        attend(1, b, 0, HALF)

        @pl.when(b == 0)
        def _():
            wo_copy.wait()

        def give_tile(n, _):
            some[_ds(row(1, b, 1 - c), HALF), _ds(n * WIDE, WIDE)] = out_dot(HALF, HALF, n).astype(BF)

        lax.fori_loop(0, downs, give_tile, None)
        far_give(b).start()
        far_give(b).wait()
        for i in range(3):

            def sum_tile(n, _):
                at = _ds(n * WIDE, WIDE)
                y = out_dot(0, HALF, n) + recv[0, _ds(b * HALF, HALF), at].astype(F32)
                hidden[_ds((3 * b + i) * HALF, HALF), _ds(TC + (n - i * third) * WIDE, WIDE)] = y.astype(BF)

            lax.fori_loop(i * third, (i + 1) * third, sum_tile, None)
            sum_over(b, i).start()

    lax.fori_loop(0, 2, far_block, None)

    for b in range(2):
        a_over(b).wait_send()
    lax.fori_loop(0, 2, lambda b, _: attend(0, b, BLOCK + b * HALF, 2 * BLOCK + b * HALF), None)

    def near_tile(n, _):
        y = out_dot(2 * BLOCK, BLOCK, n).astype(BF)
        for b in range(2):
            some[_ds(row(0, b, c), HALF), _ds(n * WIDE, WIDE)] = y[b * HALF : (b + 1) * HALF]

    lax.fori_loop(0, downs, near_tile, None)
    for b in range(2):
        near_give[b].start()
    swap[2].wait_recv()

    def b_sib(b):
        return remote(B_SIB + b, rows(some, row(0, b, c)), rows(some, sib_row(0, b, c)), sib)

    def b_over(b):
        return remote(B_OVER + b, rows(some, row(0, b, c)), rows(some, row(1, b, c)), far)

    def b_on(b):
        return remote(B_ON + b, rows(some, row(1, b, c)), rows(some, sib_row(1, b, c)), sib)

    h_swap = remote(H_SWAP, rows(x_s, BLOCK), rows(x_s, c * HALF), sib)
    for b in range(2):
        near_give[b].wait()

    def near_block(b, _):
        held = ((b + c) % 2) * BLOCK + (1 - (b + c) % 2) * c * HALF
        ours = _ds(b * HALF, HALF)
        for i in range(3):
            sum_over(b, i).wait_recv()

            def h_tile(n, _):
                at = _ds(n * WIDE, WIDE)
                y = _dot(hidden[_ds(BLOCK + b * HALF, HALF), SC : SC + 1024], hidden[:, at])
                y = x_s[_ds(held, HALF), at].astype(F32) + y + recv[1, ours, at].astype(F32)
                x_s[_ds(held, HALF), at] = (y + got[ours, at].astype(F32)).astype(BF)

            lax.fori_loop(i * third, (i + 1) * third, h_tile, None)
        norm_rows(gm_ref, held, row(0, b, c))
        b_sib(b).start()
        b_over(b).start()

    lax.fori_loop(0, 2, near_block, None)
    h_swap.start()
    for b in range(2):
        for i in range(3):
            sum_over(b, i).wait_send()
    for b in range(2):
        b_sib(b).wait_recv()

    def up_step(s, _):
        p = s % 2
        for copy in tiles_up(wg_ref, wu_ref, w, w_sem, ups, s, p):
            copy.wait()

        @pl.when(s + 1 < 2 * ups)
        def _():
            for copy in tiles_up(wg_ref, wu_ref, w, w_sem, ups, s + 1, 1 - p):
                copy.start()

        @pl.when(s + 1 == 2 * ups)
        def _():
            for copy in tiles_down(wd_ref, w, w_sem, downs, d, 0, 1 - p):
                copy.start()

        @pl.when(s == ups - 4)
        def _():
            for b in range(2):
                b_over(b).wait_recv()
                b_on(b).start()

        @pl.when(s == ups)
        def _():
            for b in range(2):
                b_on(b).wait_recv()

        at = _ds((s // ups) * (2 * BLOCK), 2 * BLOCK)
        x = some[at]
        gate, up = _dot(x, w[2 * p]), _dot(x, w[2 * p + 1])
        hidden[at, _ds((s % ups) * WIDE, WIDE)] = (jax.nn.silu(gate) * up).astype(BF)

    lax.fori_loop(0, 2 * ups, up_step, None)
    h_swap.wait_recv()
    h_swap.wait_send()
    for b in range(2):
        for copy in (b_sib(b), b_over(b), b_on(b)):
            copy.wait_send()

    def give_copy(s):
        at = _ds((s % downs) * WIDE, WIDE)
        src = some.at[_ds((1 + s // downs) * BLOCK, BLOCK), at]
        return remote(DOWN_GIVE + s, src, recv.at[s // downs, :, at], sib)

    def down_sum(n):
        at = _ds(n * WIDE, WIDE)
        return remote(DOWN_SUM + n, some.at[pl.ds(0, BLOCK), at], got.at[:, at], far)

    def out_copy(n):
        at = _ds(n * WIDE, WIDE)
        return pltpu.make_async_copy(some.at[pl.ds(3 * BLOCK, BLOCK), at], o_ref.at[:, at], o_sem.at[n])

    def finish(s):
        give_copy(s).wait_recv()
        n = s % downs
        at = _ds(n * WIDE, WIDE)

        @pl.when(s < downs)
        def _():
            some[:BLOCK, at] = (keep[s % 2] + recv[0, :, at].astype(F32)).astype(BF)
            down_sum(n).start()

        @pl.when(s >= downs)
        def _():
            down_sum(n).wait_recv()
            y = x_s[:BLOCK, at].astype(F32) + keep[s % 2] + recv[1, :, at].astype(F32) + got[:, at].astype(F32)
            some[3 * BLOCK :, at] = y.astype(BF)
            out_copy(n).start()

    def down_step(s, _):
        p = s % 2
        for copy in tiles_down(wd_ref, w, w_sem, downs, d, s, p):
            copy.wait()

        @pl.when(s + 1 < 2 * downs)
        def _():
            for copy in tiles_down(wd_ref, w, w_sem, downs, d, s + 1, 1 - p):
                copy.start()

        @pl.when(s >= 1)
        def _():
            finish(s - 1)

        at = _ds((1 - s // downs) * (2 * BLOCK), 2 * BLOCK)
        y = _dot(hidden[at, :d], w[2 * p]) + _dot(hidden[at, d:], w[2 * p + 1])
        some[_ds((1 + s // downs) * BLOCK, BLOCK), _ds((s % downs) * WIDE, WIDE)] = y[BLOCK:].astype(BF)
        keep[s % 2] = y[:BLOCK]
        give_copy(s).start()

    lax.fori_loop(0, 2 * downs, down_step, None)
    finish(2 * downs - 1)
    for n in range(downs):
        out_copy(n).wait()
        down_sum(n).wait_send()
    for s in range(2 * downs):
        give_copy(s).wait_send()


def tiles_up(wg_ref, wu_ref, w, w_sem, ups, s, p):
    at = _ds((s % ups) * WIDE, WIDE)
    return [pltpu.make_async_copy(ref.at[:, at], w.at[2 * p + i], w_sem.at[2 * p + i]) for i, ref in enumerate((wg_ref, wu_ref))]


def tiles_down(wd_ref, w, w_sem, downs, d, s, p):
    at = _ds((s % downs) * WIDE, WIDE)
    return [pltpu.make_async_copy(wd_ref.at[pl.ds(i * d, d), at], w.at[2 * p + i], w_sem.at[2 * p + i]) for i in range(2)]


def _table(tokens):
    half = HEAD // 2
    angle = np.arange(tokens)[:, None] * float(THETA) ** (-np.arange(half) / half)
    return np.concatenate([np.cos(angle), np.sin(angle)], 1).astype(np.float32)


def layer(x, gain_a, wq, wk, wv, wo, gain_m, wg, wu, wd):
    d, n = wg.shape
    dma = pltpu.SemaphoreType.DMA
    any_, vmem = pl.BlockSpec(memory_space=pl.ANY), pl.BlockSpec(memory_space=pltpu.VMEM)
    return pl.pallas_call(
        _kernel, name="layer",
        in_specs=[any_, vmem, any_, any_, any_, any_, any_, vmem, any_, any_, any_],
        out_specs=any_,
        out_shape=jax.ShapeDtypeStruct((BLOCK, d), BF),
        scratch_shapes=[
            pltpu.VMEM((4 * BLOCK, d), BF), pltpu.VMEM((4 * BLOCK, n), BF), pltpu.VMEM((4, d, WIDE), BF),
            pltpu.VMEM((2, BLOCK, d), BF), pltpu.VMEM((BLOCK, d), BF), pltpu.VMEM((2, BLOCK, WIDE), F32), pltpu.VMEM((BLOCK + HALF, d), BF),
            pltpu.VMEM((BLOCK, HEAD), F32), pltpu.VMEM((4, WIDE), F32), pltpu.VMEM((4, 8, WIDE), F32),
            dma(()), dma((4,)), dma(()), dma(()), dma((d // WIDE,)), dma((COPIES,)), dma((COPIES,)),
        ],
        compiler_params=pltpu.CompilerParams(collective_id=1, has_side_effects=True, vmem_limit_bytes=67043328),
    )(x, gain_a, jnp.asarray(_table(4 * BLOCK)), wq, wk, wv, wo, gain_m, wg, wu, wd)


def solution(mesh):
    tokens, columns, rows_of = P(("dp", "tp"), None), P(None, "tp"), P("tp", None)
    return jax.shard_map(
        layer,
        mesh=mesh,
        in_specs=(tokens, P(None), columns, columns, columns, rows_of, P(None), columns, columns, rows_of),
        out_specs=tokens,
        check_vma=False,
    )
```

```python
import jax
import jax.numpy as jnp
import numpy as np
from jax import lax
from jax.experimental import pallas as pl
from jax.experimental.pallas import tpu as pltpu
from jax.sharding import PartitionSpec as P

HEAD = 128
THETA = 10000
BLOCK = 256
HALF = 128
WIDE = 512
NEG = -1e30
LOG2E = 1.4426950408889634
BF, F32 = jnp.bfloat16, jnp.float32


SWAP, A_OVER, A_ON, FAR_GIVE, SUM, NEAR_GIVE, B_SIB, B_OVER, B_ON, H_SWAP, DOWN_GIVE, DOWN_SUM = 0, 3, 5, 7, 9, 15, 17, 19, 21, 23, 24, 42
COPIES = 51
EARLY = 4


def _dot(a, b, ca=1, cb=0):
    return lax.dot_general(a, b, (((ca,), (cb,)), ((), ())), preferred_element_type=F32)


def _ds(at, size, unit=None):
    return pl.ds(at if isinstance(at, int) else pl.multiple_of(at, unit or size), size)


def _kernel(x_ref, ga_ref, tab_ref, wq_ref, wk_ref, wv_ref, wo_ref, gm_ref, wg_ref, wu_ref, wd_ref, o_ref,
            some, hidden, w, recv, got, keep, x_s, tab_s, top_s, total_s, x_sem, w_sem, wo_sem, tab_sem, o_sem, send_sem, recv_sem):
    d = some.shape[1]
    ups, downs = wg_ref.shape[1] // WIDE, d // WIDE
    QC, KC, VC, SC, TC = d, d + 1024, d + 1536, d + 2048, d + 3072
    t = lax.axis_index("tp")
    c, chip = t % 2, t // 2
    sib, far = t + 1 - 2 * c, (t + 2) % 4

    def row(side, b, half=0):
        return side * 2 * BLOCK + ((b + c) % 2) * BLOCK + half * HALF

    def sib_row(side, b, half=0):
        return side * 2 * BLOCK + ((b + 1 + c) % 2) * BLOCK + half * HALF

    def remote(i, src, dst, to):
        return pltpu.make_async_remote_copy(src_ref=src, dst_ref=dst, send_sem=send_sem.at[i], recv_sem=recv_sem.at[i], device_id={"tp": to},
                                            device_id_type=pl.DeviceIdType.MESH)

    def rows(ref, at, size=HALF):
        return ref.at[_ds(at, size, HALF)]

    barrier = pltpu.get_barrier_semaphore()
    for to in (sib, far):
        pl.semaphore_signal(barrier, inc=1, device_id={"tp": to}, device_id_type=pl.DeviceIdType.MESH)
    other, mine = (1 - c) * HALF, c * HALF
    loads = [pltpu.make_async_copy(rows(x_ref, at), rows(x_s, at), x_sem.at[i]) for i, at in enumerate((mine, other))]
    in_weights = [pltpu.make_async_copy(src, w.at[i], w_sem.at[i]) for i, src in
                  enumerate((wq_ref.at[:, pl.ds(0, WIDE)], wq_ref.at[:, pl.ds(WIDE, WIDE)], wk_ref, wv_ref))]
    wo_copy = pltpu.make_async_copy(wo_ref, hidden.at[:, pl.ds(0, d)], wo_sem)
    for copy in loads:
        copy.start()
    for copy in loads:
        copy.wait()
    for copy in in_weights:
        copy.start()
    wo_copy.start()

    def norm_rows(gain_ref, src, dst):
        gain = gain_ref[...].astype(F32)[None]

        def go(i, _):
            wide = x_s[_ds(src + i * 32, 32)].astype(F32)
            scale = lax.rsqrt(jnp.mean(wide * wide, -1, keepdims=True) + 1e-6)
            some[_ds(dst + i * 32, 32)] = (wide * scale * gain).astype(BF)

        lax.fori_loop(0, HALF // 32, go, None)

    swap = [remote(SWAP, rows(some, other), rows(some, BLOCK + other), sib),
            remote(SWAP + 1, rows(some, mine), rows(some, BLOCK + mine), sib),
            remote(SWAP + 2, rows(x_s, other), rows(x_s, BLOCK), sib)]

    def a_over(b):
        return remote(A_OVER + b, rows(some, row(0, b, c)), rows(some, row(1, b, c)), far)

    def a_on(b):
        return remote(A_ON + b, rows(some, row(1, b, c)), rows(some, sib_row(1, b, c)), sib)

    norm_rows(ga_ref, mine, mine)
    pl.semaphore_wait(barrier, 2)

    @pl.when(c == 0)
    def _():
        a_over(0).start()

    norm_rows(ga_ref, other, other)
    swap[0].start()
    swap[1].start()
    swap[2].start()
    swap[0].wait_recv()

    @pl.when(c == 1)
    def _():
        a_over(0).start()

    a_over(1).start()

    def table_copy(i):
        place = ((chip + i // 2) % 2) * 2 + i % 2
        return pltpu.make_async_copy(tab_ref.at[_ds(place * BLOCK, BLOCK)], tab_s, tab_sem)

    def qkv(side, b):
        at = _ds(row(side, b), BLOCK)
        table_copy(side * 2 + b).wait()
        table = tab_s[...]
        turned = pltpu.roll(table, HEAD // 2, 1)
        first = lax.broadcasted_iota(jnp.int32, table.shape, 1) < HEAD // 2
        cos, sin = jnp.where(first, table, turned), jnp.where(first, -turned, table)
        for i, to in enumerate((QC, QC + WIDE, KC, VC)):
            y = _dot(some[at], w[i]).astype(BF)
            if i < 3:
                heads = []
                for n in range(WIDE // HEAD):
                    u = y[:, n * HEAD : (n + 1) * HEAD].astype(F32)
                    heads.append((u * cos + pltpu.roll(u, HEAD // 2, 1) * sin).astype(BF))
                y = jnp.concatenate(heads, 1)
            hidden[at, to : to + WIDE] = y

        @pl.when(side * 2 + b < 3)
        def _():
            table_copy(side * 2 + b + 1).start()

    groups, g = WIDE // HEAD, 2
    cols = g * BLOCK
    e = HEAD**-0.5 * LOG2E
    ones = jnp.ones((8, BLOCK), BF)

    def attend(side, b, kept, given):
        at = _ds(row(side, b), BLOCK)
        top_s[...] = jnp.full(top_s.shape, NEG, F32)
        total_s[...] = jnp.zeros(total_s.shape, F32)
        keep[...] = jnp.zeros(keep.shape, F32)

        def block(key_row, masked):
            here = _ds(key_row, BLOCK)
            weights, shrinks = [], []
            for i in range(groups):
                q = jnp.concatenate([hidden[at, QC + (g * i + n) * HEAD : QC + (g * i + n + 1) * HEAD] for n in range(g)], 0)
                s = _dot(hidden[here, KC + i * HEAD : KC + (i + 1) * HEAD], q, 1, 1)
                if masked:
                    gap = lax.broadcasted_iota(jnp.int32, s.shape, 1) % BLOCK - lax.broadcasted_iota(jnp.int32, s.shape, 0)
                    s = jnp.where(gap >= 0, s, 2 * NEG)
                old = top_s[i : i + 1, :]
                top = jnp.maximum(old, s.max(axis=0, keepdims=True))
                top_s[i : i + 1, :] = top
                weights.append(jnp.exp2((s - top) * e).astype(BF))
                shrinks.append(jnp.exp2((old - top) * e))
            for i, (p, shrink) in enumerate(zip(weights, shrinks)):
                values = jnp.concatenate([hidden[here, VC + i * HEAD : VC + (i + 1) * HEAD].T, ones], axis=0)
                more = _dot(values, p)
                to = slice((i % 2) * HEAD, (i % 2 + 1) * HEAD)
                keep[i // 2, to] = keep[i // 2, to] * shrink + more[:HEAD]
                total_s[i] = total_s[i] * shrink + more[HEAD:]

        before = 2 * (1 - chip) if side else 2 * chip

        def whole(j, _):
            there = (before // 2) * (1 - j // 2)
            block(there * ((1 - side) * 2 * BLOCK + j * BLOCK) + (1 - there) * row(side, 0), False)

        lax.fori_loop(0, before + b, whole, None)
        block(row(side, b), True)
        for i in range(groups):
            out = (keep[i // 2, (i % 2) * HEAD : (i % 2 + 1) * HEAD] * (1 / total_s[i, :1])).T.astype(BF)
            for n in range(g):
                to = slice(SC + (g * i + n) * HEAD, SC + (g * i + n + 1) * HEAD)
                for half in range(2):
                    piece = out[n * BLOCK + half * HALF : n * BLOCK + (half + 1) * HALF]
                    hidden[_ds(kept + ((half + c) % 2) * (given - kept), HALF), to] = piece

    def out_dot(at, size, n):
        return _dot(hidden[at : at + size, SC : SC + 1024], hidden[:, _ds(n * WIDE, WIDE)])

    table_copy(0).start()
    for copy in in_weights:
        copy.wait()
    swap[1].wait_recv()
    lax.fori_loop(0, 2, lambda b, _: qkv(0, b), None)
    for copy in swap:
        copy.wait_send()

    def far_give(b):
        return remote(FAR_GIVE + b, rows(some, row(1, b, 1 - c)), rows(recv.at[0], b * HALF), sib)

    near_give = [remote(NEAR_GIVE + b, rows(some, row(0, b, c)), rows(recv.at[1], b * HALF), sib) for b in range(2)]
    third = downs // 3

    def sum_over(b, i):
        part = pl.ds(i * third * WIDE, third * WIDE)
        return remote(SUM + 3 * b + i, hidden.at[_ds((3 * b + i) * HALF, HALF), pl.ds(TC, third * WIDE)], got.at[_ds(b * HALF, HALF), part], far)

    def far_block(b, _):
        a_over(b).wait_recv()
        a_on(b).start()
        a_on(b).wait_recv()
        qkv(1, b)
        a_on(b).wait_send()

        @pl.when(b == 1)
        def _():
            for copy in tiles_up(wg_ref, wu_ref, w, w_sem, ups, 0, 0):
                copy.start()

        attend(1, b, 0, HALF)

        @pl.when(b == 0)
        def _():
            wo_copy.wait()

        def give_tile(n, _):
            some[_ds(row(1, b, 1 - c), HALF), _ds(n * WIDE, WIDE)] = out_dot(HALF, HALF, n).astype(BF)

        lax.fori_loop(0, downs, give_tile, None)
        far_give(b).start()
        far_give(b).wait()

        @pl.when(b == 0)
        def _():
            a_over(1).wait_send()

        for i in range(3):

            def sum_tile(n, _):
                at = _ds(n * WIDE, WIDE)
                y = out_dot(0, HALF, n) + recv[0, _ds(b * HALF, HALF), at].astype(F32)
                hidden[_ds((3 * b + i) * HALF, HALF), _ds(TC + (n - i * third) * WIDE, WIDE)] = y.astype(BF)

            lax.fori_loop(i * third, (i + 1) * third, sum_tile, None)
            sum_over(b, i).start()

    lax.fori_loop(0, 2, far_block, None)

    a_over(0).wait_send()
    lax.fori_loop(0, 2, lambda b, _: attend(0, b, 2 * BLOCK + b * HALF, 3 * BLOCK + b * HALF), None)

    def near_tile(n, _):
        y = out_dot(3 * BLOCK, BLOCK, n).astype(BF)
        for b in range(2):
            some[_ds(row(0, b, c), HALF), _ds(n * WIDE, WIDE)] = y[b * HALF : (b + 1) * HALF]

    lax.fori_loop(0, downs, near_tile, None)
    for b in range(2):
        near_give[b].start()
    swap[2].wait_recv()

    def b_sib(b):
        return remote(B_SIB + b, rows(some, row(0, b, c)), rows(some, sib_row(0, b, c)), sib)

    def b_over(b):
        return remote(B_OVER + b, rows(some, row(0, b, c)), rows(some, row(1, b, c)), far)

    def b_on(b):
        return remote(B_ON + b, rows(some, row(1, b, c)), rows(some, sib_row(1, b, c)), sib)

    h_swap = remote(H_SWAP, rows(x_s, BLOCK), rows(x_s, c * HALF), sib)
    for b in range(2):
        near_give[b].wait()

    def near_block(b):
        held = ((b + c) % 2) * BLOCK + (1 - (b + c) % 2) * c * HALF
        ours = _ds(b * HALF, HALF)
        for i in range(3):
            sum_over(b, i).wait_recv()

            def h_tile(n, _):
                at = _ds(n * WIDE, WIDE)
                y = _dot(hidden[_ds(2 * BLOCK + b * HALF, HALF), SC : SC + 1024], hidden[:, at])
                y = x_s[_ds(held, HALF), at].astype(F32) + y + recv[1, ours, at].astype(F32)
                x_s[_ds(held, HALF), at] = (y + got[ours, at].astype(F32)).astype(BF)

            lax.fori_loop(i * third, (i + 1) * third, h_tile, None)
        norm_rows(gm_ref, held, row(0, b, c))
        b_sib(b).start()
        b_over(b).start()

    def up_tiles(s):
        p = s % 2
        for copy in tiles_up(wg_ref, wu_ref, w, w_sem, ups, s, p):
            copy.wait()

        @pl.when(s + 1 < 2 * ups)
        def _():
            for copy in tiles_up(wg_ref, wu_ref, w, w_sem, ups, s + 1, 1 - p):
                copy.start()

        @pl.when(s + 1 == 2 * ups)
        def _():
            for copy in tiles_down(wd_ref, w, w_sem, downs, d, 0, 1 - p):
                copy.start()

    def up_rows(s, at, size):
        p, at = s % 2, _ds(at, size)
        x = some[at]
        gate, up = _dot(x, w[2 * p]), _dot(x, w[2 * p + 1])
        hidden[at, _ds(up_tile(s, ups) * WIDE, WIDE)] = (jax.nn.silu(gate) * up).astype(BF)

    def up_step(s, _):
        @pl.when((s == 0) | (s == EARLY))
        def _():
            near_block(s // EARLY)
            b_sib(s // EARLY).wait_recv()

        @pl.when(s == EARLY)
        def _():
            h_swap.start()
            for b in range(2):
                for i in range(3):
                    sum_over(b, i).wait_send()

        up_tiles(s)

        @pl.when(s == ups - 4)
        def _():
            for b in range(2):
                b_over(b).wait_recv()
                b_on(b).start()

        @pl.when(s == ups)
        def _():
            for b in range(2):
                b_on(b).wait_recv()

        @pl.when(s % ups < EARLY)
        def _():
            up_rows(s, row(0, s // ups), BLOCK)

        @pl.when(s >= EARLY)
        def _():
            up_rows(s, (s // ups) * (2 * BLOCK), 2 * BLOCK)

    lax.fori_loop(0, 2 * ups, up_step, None)
    h_swap.wait_recv()
    h_swap.wait_send()
    for b in range(2):
        for copy in (b_sib(b), b_over(b), b_on(b)):
            copy.wait_send()

    def give_copy(s):
        at = _ds((s % downs) * WIDE, WIDE)
        src = some.at[_ds((1 + s // downs) * BLOCK, BLOCK), at]
        return remote(DOWN_GIVE + s, src, recv.at[s // downs, :, at], sib)

    def down_sum(n):
        at = _ds(n * WIDE, WIDE)
        return remote(DOWN_SUM + n, some.at[pl.ds(0, BLOCK), at], got.at[:, at], far)

    def out_copy(n):
        at = _ds(n * WIDE, WIDE)
        return pltpu.make_async_copy(some.at[pl.ds(3 * BLOCK, BLOCK), at], o_ref.at[:, at], o_sem.at[n])

    def finish(s):
        give_copy(s).wait_recv()
        n = s % downs
        at = _ds(n * WIDE, WIDE)

        @pl.when(s < downs)
        def _():
            some[:BLOCK, at] = (keep[s % 2] + recv[0, :, at].astype(F32)).astype(BF)
            down_sum(n).start()

        @pl.when(s >= downs)
        def _():
            down_sum(n).wait_recv()
            y = x_s[:BLOCK, at].astype(F32) + keep[s % 2] + recv[1, :, at].astype(F32) + got[:, at].astype(F32)
            some[3 * BLOCK :, at] = y.astype(BF)
            out_copy(n).start()

    def down_step(s, _):
        p = s % 2
        for copy in tiles_down(wd_ref, w, w_sem, downs, d, s, p):
            copy.wait()

        @pl.when(s + 1 < 2 * downs)
        def _():
            for copy in tiles_down(wd_ref, w, w_sem, downs, d, s + 1, 1 - p):
                copy.start()

        @pl.when(s >= 1)
        def _():
            finish(s - 1)

        at = _ds((1 - s // downs) * (2 * BLOCK), 2 * BLOCK)
        y = _dot(hidden[at, :d], w[2 * p]) + _dot(hidden[at, d:], w[2 * p + 1])
        some[_ds((1 + s // downs) * BLOCK, BLOCK), _ds((s % downs) * WIDE, WIDE)] = y[BLOCK:].astype(BF)
        keep[s % 2] = y[:BLOCK]
        give_copy(s).start()

    lax.fori_loop(0, 2 * downs, down_step, None)
    finish(2 * downs - 1)
    for n in range(downs):
        out_copy(n).wait()
        down_sum(n).wait_send()
    for s in range(2 * downs):
        give_copy(s).wait_send()


def up_tile(s, ups):
    return (s + ups // 2) % ups


def tiles_up(wg_ref, wu_ref, w, w_sem, ups, s, p):
    at = _ds(up_tile(s, ups) * WIDE, WIDE)
    return [pltpu.make_async_copy(ref.at[:, at], w.at[2 * p + i], w_sem.at[2 * p + i]) for i, ref in enumerate((wg_ref, wu_ref))]


def tiles_down(wd_ref, w, w_sem, downs, d, s, p):
    at = _ds((s % downs) * WIDE, WIDE)
    return [pltpu.make_async_copy(wd_ref.at[pl.ds(i * d, d), at], w.at[2 * p + i], w_sem.at[2 * p + i]) for i in range(2)]


def _table(tokens):
    half = HEAD // 2
    angle = np.arange(tokens)[:, None] * float(THETA) ** (-np.arange(half) / half)
    return np.concatenate([np.cos(angle), np.sin(angle)], 1).astype(np.float32)


def layer(x, gain_a, wq, wk, wv, wo, gain_m, wg, wu, wd):
    d, n = wg.shape
    dma = pltpu.SemaphoreType.DMA
    any_, vmem = pl.BlockSpec(memory_space=pl.ANY), pl.BlockSpec(memory_space=pltpu.VMEM)
    return pl.pallas_call(
        _kernel, name="layer",
        in_specs=[any_, vmem, any_, any_, any_, any_, any_, vmem, any_, any_, any_],
        out_specs=any_,
        out_shape=jax.ShapeDtypeStruct((BLOCK, d), BF),
        scratch_shapes=[
            pltpu.VMEM((4 * BLOCK, d), BF), pltpu.VMEM((4 * BLOCK, n), BF), pltpu.VMEM((4, d, WIDE), BF),
            pltpu.VMEM((2, BLOCK, d), BF), pltpu.VMEM((BLOCK, d), BF), pltpu.VMEM((2, BLOCK, WIDE), F32), pltpu.VMEM((BLOCK + HALF, d), BF),
            pltpu.VMEM((BLOCK, HEAD), F32), pltpu.VMEM((4, WIDE), F32), pltpu.VMEM((4, 8, WIDE), F32),
            dma((2,)), dma((4,)), dma(()), dma(()), dma((d // WIDE,)), dma((COPIES,)), dma((COPIES,)),
        ],
        compiler_params=pltpu.CompilerParams(collective_id=1, has_side_effects=True, vmem_limit_bytes=67043328),
    )(x, gain_a, jnp.asarray(_table(4 * BLOCK)), wq, wk, wv, wo, gain_m, wg, wu, wd)


def solution(mesh):
    tokens, columns, rows_of = P(("dp", "tp"), None), P(None, "tp"), P("tp", None)
    return jax.shard_map(
        layer,
        mesh=mesh,
        in_specs=(tokens, P(None), columns, columns, columns, rows_of, P(None), columns, columns, rows_of),
        out_specs=tokens,
        check_vma=False,
    )
```

```python
import jax
import jax.numpy as jnp
import numpy as np
from jax import lax
from jax.experimental import pallas as pl
from jax.experimental.pallas import tpu as pltpu
from jax.sharding import PartitionSpec as P

HEAD = 128
THETA = 10000
BLOCK = 256
HALF = 128
WIDE = 512
NEG = -1e30
LOG2E = 1.4426950408889634
BF, F32 = jnp.bfloat16, jnp.float32


SWAP, A_OVER, A_ON, FAR_GIVE, SUM, NEAR_GIVE, B_SIB, B_OVER, B_ON, H_SWAP, DOWN_GIVE, DOWN_SUM = 0, 3, 5, 7, 9, 15, 17, 19, 21, 23, 24, 42
COPIES = 51
EARLY = 4


def _dot(a, b, ca=1, cb=0):
    return lax.dot_general(a, b, (((ca,), (cb,)), ((), ())), preferred_element_type=F32)


def _ds(at, size, unit=None):
    return pl.ds(at if isinstance(at, int) else pl.multiple_of(at, unit or size), size)


def _kernel(x_ref, ga_ref, tab_ref, wq_ref, wk_ref, wv_ref, wo_ref, gm_ref, wg_ref, wu_ref, wd_ref, o_ref,
            some, hidden, w, recv, got, keep, x_s, tab_s, top_s, total_s, x_sem, w_sem, wo_sem, tab_sem, o_sem, send_sem, recv_sem):
    d = some.shape[1]
    ups, downs = wg_ref.shape[1] // WIDE, d // WIDE
    QC, KC, VC, SC, TC = d, d + 1024, d + 1536, d + 2048, d + 3072
    t = lax.axis_index("tp")
    c, chip = t % 2, t // 2
    sib, far = t + 1 - 2 * c, (t + 2) % 4

    def row(side, b, half=0):
        return side * 2 * BLOCK + ((b + c) % 2) * BLOCK + half * HALF

    def sib_row(side, b, half=0):
        return side * 2 * BLOCK + ((b + 1 + c) % 2) * BLOCK + half * HALF

    def remote(i, src, dst, to):
        return pltpu.make_async_remote_copy(src_ref=src, dst_ref=dst, send_sem=send_sem.at[i], recv_sem=recv_sem.at[i], device_id={"tp": to},
                                            device_id_type=pl.DeviceIdType.MESH)

    def rows(ref, at, size=HALF):
        return ref.at[_ds(at, size, HALF)]

    barrier = pltpu.get_barrier_semaphore()
    for to in (sib, far):
        pl.semaphore_signal(barrier, inc=1, device_id={"tp": to}, device_id_type=pl.DeviceIdType.MESH)
    other, mine = (1 - c) * HALF, c * HALF
    loads = [pltpu.make_async_copy(rows(x_ref, at), rows(x_s, at), x_sem.at[i]) for i, at in enumerate((mine, other))]
    in_weights = [pltpu.make_async_copy(src, w.at[i], w_sem.at[i]) for i, src in
                  enumerate((wq_ref.at[:, pl.ds(0, WIDE)], wq_ref.at[:, pl.ds(WIDE, WIDE)], wk_ref, wv_ref))]
    wo_copy = pltpu.make_async_copy(wo_ref, hidden.at[:, pl.ds(0, d)], wo_sem)
    for copy in loads:
        copy.start()
    for copy in loads:
        copy.wait()
    for copy in in_weights:
        copy.start()
    wo_copy.start()

    def norm_rows(gain_ref, src, dst):
        gain = gain_ref[...].astype(F32)[None]

        def go(i, _):
            wide = x_s[_ds(src + i * 32, 32)].astype(F32)
            scale = lax.rsqrt(jnp.mean(wide * wide, -1, keepdims=True) + 1e-6)
            some[_ds(dst + i * 32, 32)] = (wide * scale * gain).astype(BF)

        lax.fori_loop(0, HALF // 32, go, None)

    swap = [remote(SWAP, rows(some, other), rows(some, BLOCK + other), sib),
            remote(SWAP + 1, rows(some, mine), rows(some, BLOCK + mine), sib),
            remote(SWAP + 2, rows(x_s, other), rows(x_s, BLOCK), sib)]

    def a_over(b):
        return remote(A_OVER + b, rows(some, row(0, b, c)), rows(some, row(1, b, c)), far)

    def a_on(b):
        return remote(A_ON + b, rows(some, row(1, b, c)), rows(some, sib_row(1, b, c)), sib)

    norm_rows(ga_ref, mine, mine)
    pl.semaphore_wait(barrier, 2)

    @pl.when(c == 0)
    def _():
        a_over(0).start()

    norm_rows(ga_ref, other, other)
    swap[0].start()
    swap[1].start()
    swap[2].start()
    swap[0].wait_recv()

    @pl.when(c == 1)
    def _():
        a_over(0).start()

    a_over(1).start()

    def tiles(first, last, body):
        for n in range(first, last):
            body(n)

    def table_copy(i):
        place = ((chip + i // 2) % 2) * 2 + i % 2
        return pltpu.make_async_copy(tab_ref.at[_ds(place * BLOCK, BLOCK)], tab_s, tab_sem)

    def qkv(side, b):
        at = _ds(row(side, b), BLOCK)
        table_copy(side * 2 + b).wait()
        table = tab_s[...]
        turned = pltpu.roll(table, HEAD // 2, 1)
        first = lax.broadcasted_iota(jnp.int32, table.shape, 1) < HEAD // 2
        cos, sin = jnp.where(first, table, turned), jnp.where(first, -turned, table)
        for i, to in enumerate((QC, QC + WIDE, KC, VC)):
            y = _dot(some[at], w[i]).astype(BF)
            if i < 3:
                heads = []
                for n in range(WIDE // HEAD):
                    u = y[:, n * HEAD : (n + 1) * HEAD].astype(F32)
                    heads.append((u * cos + pltpu.roll(u, HEAD // 2, 1) * sin).astype(BF))
                y = jnp.concatenate(heads, 1)
            hidden[at, to : to + WIDE] = y

        @pl.when(side * 2 + b < 3)
        def _():
            table_copy(side * 2 + b + 1).start()

    groups, g = WIDE // HEAD, 2
    cols = g * BLOCK
    e = HEAD**-0.5 * LOG2E
    ones = jnp.ones((8, BLOCK), BF)

    def attend(side, b, kept, given):
        at = _ds(row(side, b), BLOCK)
        top_s[...] = jnp.full(top_s.shape, NEG, F32)
        total_s[...] = jnp.zeros(total_s.shape, F32)
        keep[...] = jnp.zeros(keep.shape, F32)

        def block(key_row, masked):
            here = _ds(key_row, BLOCK)
            weights, shrinks = [], []
            for i in range(groups):
                q = jnp.concatenate([hidden[at, QC + (g * i + n) * HEAD : QC + (g * i + n + 1) * HEAD] for n in range(g)], 0)
                s = _dot(hidden[here, KC + i * HEAD : KC + (i + 1) * HEAD], q, 1, 1)
                if masked:
                    gap = lax.broadcasted_iota(jnp.int32, s.shape, 1) % BLOCK - lax.broadcasted_iota(jnp.int32, s.shape, 0)
                    s = jnp.where(gap >= 0, s, 2 * NEG)
                old = top_s[i : i + 1, :]
                top = jnp.maximum(old, s.max(axis=0, keepdims=True))
                top_s[i : i + 1, :] = top
                weights.append(jnp.exp2((s - top) * e).astype(BF))
                shrinks.append(jnp.exp2((old - top) * e))
            for i, (p, shrink) in enumerate(zip(weights, shrinks)):
                values = jnp.concatenate([hidden[here, VC + i * HEAD : VC + (i + 1) * HEAD].T, ones], axis=0)
                more = _dot(values, p)
                to = slice((i % 2) * HEAD, (i % 2 + 1) * HEAD)
                keep[i // 2, to] = keep[i // 2, to] * shrink + more[:HEAD]
                total_s[i] = total_s[i] * shrink + more[HEAD:]

        before = 2 * (1 - chip) if side else 2 * chip

        def whole(j, _):
            there = (before // 2) * (1 - j // 2)
            block(there * ((1 - side) * 2 * BLOCK + j * BLOCK) + (1 - there) * row(side, 0), False)

        lax.fori_loop(0, before + b, whole, None)
        block(row(side, b), True)
        for i in range(groups):
            out = (keep[i // 2, (i % 2) * HEAD : (i % 2 + 1) * HEAD] * (1 / total_s[i, :1])).T.astype(BF)
            for n in range(g):
                to = slice(SC + (g * i + n) * HEAD, SC + (g * i + n + 1) * HEAD)
                for half in range(2):
                    piece = out[n * BLOCK + half * HALF : n * BLOCK + (half + 1) * HALF]
                    hidden[_ds(kept + ((half + c) % 2) * (given - kept), HALF), to] = piece

    def out_dot(at, size, n):
        return _dot(hidden[at : at + size, SC : SC + 1024], hidden[:, _ds(n * WIDE, WIDE)])

    table_copy(0).start()
    for copy in in_weights:
        copy.wait()
    swap[1].wait_recv()
    lax.fori_loop(0, 2, lambda b, _: qkv(0, b), None)
    for copy in swap:
        copy.wait_send()

    def far_give(b):
        return remote(FAR_GIVE + b, rows(some, row(1, b, 1 - c)), rows(recv.at[0], b * HALF), sib)

    near_give = [remote(NEAR_GIVE + b, rows(some, row(0, b, c)), rows(recv.at[1], b * HALF), sib) for b in range(2)]
    third = downs // 3

    def sum_over(b, i):
        part = pl.ds(i * third * WIDE, third * WIDE)
        return remote(SUM + 3 * b + i, hidden.at[_ds((3 * b + i) * HALF, HALF), pl.ds(TC, third * WIDE)], got.at[_ds(b * HALF, HALF), part], far)

    def far_block(b, _):
        a_over(b).wait_recv()
        a_on(b).start()
        a_on(b).wait_recv()
        qkv(1, b)
        a_on(b).wait_send()

        @pl.when(b == 1)
        def _():
            for s in range(2):
                for copy in tiles_up(wg_ref, wu_ref, w, w_sem, ups, s, s):
                    copy.start()

        attend(1, b, 0, HALF)

        @pl.when(b == 0)
        def _():
            wo_copy.wait()

        def give_tile(n):
            some[_ds(row(1, b, 1 - c), HALF), _ds(n * WIDE, WIDE)] = out_dot(HALF, HALF, n).astype(BF)

        tiles(0, downs, give_tile)
        far_give(b).start()

        @pl.when(b == chip)
        def _():
            attend(0, 0, 2 * BLOCK, 3 * BLOCK)

        far_give(b).wait()

        @pl.when(b == 0)
        def _():
            a_over(1).wait_send()

        for i in range(3):

            def sum_tile(n):
                at = _ds(n * WIDE, WIDE)
                y = out_dot(0, HALF, n) + recv[0, _ds(b * HALF, HALF), at].astype(F32)
                hidden[_ds((3 * b + i) * HALF, HALF), _ds(TC + (n - i * third) * WIDE, WIDE)] = y.astype(BF)

            tiles(i * third, (i + 1) * third, sum_tile)
            sum_over(b, i).start()

    lax.fori_loop(0, 2, far_block, None)

    a_over(0).wait_send()
    attend(0, 1, 2 * BLOCK + HALF, 3 * BLOCK + HALF)

    def near_tile(n):
        y = out_dot(3 * BLOCK, BLOCK, n).astype(BF)
        for b in range(2):
            some[_ds(row(0, b, c), HALF), _ds(n * WIDE, WIDE)] = y[b * HALF : (b + 1) * HALF]

    tiles(0, downs, near_tile)
    for b in range(2):
        near_give[b].start()
    swap[2].wait_recv()

    def b_sib(b):
        return remote(B_SIB + b, rows(some, row(0, b, c)), rows(some, sib_row(0, b, c)), sib)

    def b_over(b):
        return remote(B_OVER + b, rows(some, row(0, b, c)), rows(some, row(1, b, c)), far)

    def b_on(b):
        return remote(B_ON + b, rows(some, row(1, b, c)), rows(some, sib_row(1, b, c)), sib)

    h_swap = remote(H_SWAP, rows(x_s, BLOCK), rows(x_s, c * HALF), sib)
    for b in range(2):
        near_give[b].wait()

    def near_block(b):
        held = ((b + c) % 2) * BLOCK + (1 - (b + c) % 2) * c * HALF
        ours = _ds(b * HALF, HALF)
        for i in range(3):
            sum_over(b, i).wait_recv()

            def h_tile(n):
                at = _ds(n * WIDE, WIDE)
                y = _dot(hidden[_ds(2 * BLOCK + b * HALF, HALF), SC : SC + 1024], hidden[:, at])
                y = x_s[_ds(held, HALF), at].astype(F32) + y + recv[1, ours, at].astype(F32)
                x_s[_ds(held, HALF), at] = (y + got[ours, at].astype(F32)).astype(BF)

            tiles(i * third, (i + 1) * third, h_tile)
        norm_rows(gm_ref, held, row(0, b, c))
        b_sib(b).start()
        b_over(b).start()

    def up_tiles(s):
        p = s % 2
        for copy in tiles_up(wg_ref, wu_ref, w, w_sem, ups, s, p):
            copy.wait()

        @pl.when((s >= 1) & (s + 1 < 2 * ups))
        def _():
            for copy in tiles_up(wg_ref, wu_ref, w, w_sem, ups, s + 1, 1 - p):
                copy.start()

        @pl.when(s + 1 == 2 * ups)
        def _():
            for copy in tiles_down(wd_ref, w, w_sem, downs, d, 0, 1 - p):
                copy.start()

    def up_rows(s, at, size):
        p, at = s % 2, _ds(at, size)
        x = some[at]
        gate, up = _dot(x, w[2 * p]), _dot(x, w[2 * p + 1])
        hidden[at, _ds(up_tile(s, ups) * WIDE, WIDE)] = (jax.nn.silu(gate) * up).astype(BF)

    def up_step(s, _):
        @pl.when((s == 0) | (s == EARLY))
        def _():
            near_block(s // EARLY)
            b_sib(s // EARLY).wait_recv()

        @pl.when(s == EARLY)
        def _():
            h_swap.start()
            for b in range(2):
                for i in range(3):
                    sum_over(b, i).wait_send()

        up_tiles(s)

        @pl.when(s == ups - 4)
        def _():
            for b in range(2):
                b_over(b).wait_recv()
                b_on(b).start()

        @pl.when(s == ups)
        def _():
            for b in range(2):
                b_on(b).wait_recv()

        @pl.when(s % ups < EARLY)
        def _():
            up_rows(s, row(0, s // ups), BLOCK)

        @pl.when(s >= EARLY)
        def _():
            up_rows(s, (s // ups) * (2 * BLOCK), 2 * BLOCK)

    lax.fori_loop(0, 2 * ups, up_step, None)
    h_swap.wait_recv()
    h_swap.wait_send()
    for b in range(2):
        for copy in (b_sib(b), b_over(b), b_on(b)):
            copy.wait_send()

    def give_copy(s):
        at = _ds((s % downs) * WIDE, WIDE)
        src = some.at[_ds((1 + s // downs) * BLOCK, BLOCK), at]
        return remote(DOWN_GIVE + s, src, recv.at[s // downs, :, at], sib)

    def down_sum(n):
        at = _ds(n * WIDE, WIDE)
        return remote(DOWN_SUM + n, some.at[pl.ds(0, BLOCK), at], got.at[:, at], far)

    def out_copy(n):
        at = _ds(n * WIDE, WIDE)
        return pltpu.make_async_copy(some.at[pl.ds(3 * BLOCK, BLOCK), at], o_ref.at[:, at], o_sem.at[n])

    def finish(s):
        give_copy(s).wait_recv()
        n = s % downs
        at = _ds(n * WIDE, WIDE)

        @pl.when(s < downs)
        def _():
            some[:BLOCK, at] = (keep[s % 2] + recv[0, :, at].astype(F32)).astype(BF)
            down_sum(n).start()

        @pl.when(s >= downs)
        def _():
            down_sum(n).wait_recv()
            y = x_s[:BLOCK, at].astype(F32) + keep[s % 2] + recv[1, :, at].astype(F32) + got[:, at].astype(F32)
            some[3 * BLOCK :, at] = y.astype(BF)
            out_copy(n).start()

    def down_step(s, _):
        p = s % 2
        for copy in tiles_down(wd_ref, w, w_sem, downs, d, s, p):
            copy.wait()

        @pl.when(s + 1 < 2 * downs)
        def _():
            for copy in tiles_down(wd_ref, w, w_sem, downs, d, s + 1, 1 - p):
                copy.start()

        @pl.when(s >= 1)
        def _():
            finish(s - 1)

        at = _ds((1 - s // downs) * (2 * BLOCK), 2 * BLOCK)
        y = _dot(hidden[at, :d], w[2 * p]) + _dot(hidden[at, d:], w[2 * p + 1])
        some[_ds((1 + s // downs) * BLOCK, BLOCK), _ds((s % downs) * WIDE, WIDE)] = y[BLOCK:].astype(BF)
        keep[s % 2] = y[:BLOCK]
        give_copy(s).start()

    lax.fori_loop(0, 2 * downs, down_step, None)
    finish(2 * downs - 1)
    for n in range(downs):
        out_copy(n).wait()
        down_sum(n).wait_send()
    for s in range(2 * downs):
        give_copy(s).wait_send()


def up_tile(s, ups):
    return (s + ups // 2) % ups


def tiles_up(wg_ref, wu_ref, w, w_sem, ups, s, p):
    at = _ds(up_tile(s, ups) * WIDE, WIDE)
    return [pltpu.make_async_copy(ref.at[:, at], w.at[2 * p + i], w_sem.at[2 * p + i]) for i, ref in enumerate((wg_ref, wu_ref))]


def tiles_down(wd_ref, w, w_sem, downs, d, s, p):
    at = _ds((s % downs) * WIDE, WIDE)
    return [pltpu.make_async_copy(wd_ref.at[pl.ds(i * d, d), at], w.at[2 * p + i], w_sem.at[2 * p + i]) for i in range(2)]


def _table(tokens):
    half = HEAD // 2
    angle = np.arange(tokens)[:, None] * float(THETA) ** (-np.arange(half) / half)
    return np.concatenate([np.cos(angle), np.sin(angle)], 1).astype(np.float32)


def layer(x, gain_a, wq, wk, wv, wo, gain_m, wg, wu, wd):
    d, n = wg.shape
    dma = pltpu.SemaphoreType.DMA
    any_, vmem = pl.BlockSpec(memory_space=pl.ANY), pl.BlockSpec(memory_space=pltpu.VMEM)
    return pl.pallas_call(
        _kernel, name="layer",
        in_specs=[any_, vmem, any_, any_, any_, any_, any_, vmem, any_, any_, any_],
        out_specs=any_,
        out_shape=jax.ShapeDtypeStruct((BLOCK, d), BF),
        scratch_shapes=[
            pltpu.VMEM((4 * BLOCK, d), BF), pltpu.VMEM((4 * BLOCK, n), BF), pltpu.VMEM((4, d, WIDE), BF),
            pltpu.VMEM((2, BLOCK, d), BF), pltpu.VMEM((BLOCK, d), BF), pltpu.VMEM((2, BLOCK, WIDE), F32), pltpu.VMEM((BLOCK + HALF, d), BF),
            pltpu.VMEM((BLOCK, HEAD), F32), pltpu.VMEM((4, WIDE), F32), pltpu.VMEM((4, 8, WIDE), F32),
            dma((2,)), dma((4,)), dma(()), dma(()), dma((d // WIDE,)), dma((COPIES,)), dma((COPIES,)),
        ],
        compiler_params=pltpu.CompilerParams(collective_id=1, has_side_effects=True, vmem_limit_bytes=67043328),
    )(x, gain_a, jnp.asarray(_table(4 * BLOCK)), wq, wk, wv, wo, gain_m, wg, wu, wd)


def solution(mesh):
    tokens, columns, rows_of = P(("dp", "tp"), None), P(None, "tp"), P("tp", None)
    return jax.shard_map(
        layer,
        mesh=mesh,
        in_specs=(tokens, P(None), columns, columns, columns, rows_of, P(None), columns, columns, rows_of),
        out_specs=tokens,
        check_vma=False,
    )
```
